32 devices in a mesh: dp: 8 (over y, x, core), seq: 4 (over z).
Axes of the slice: x: 2, y: 2, z: 4, core: 2. Of those that a mesh axis runs over, the one named last changes fastest.
Arguments:
- tile_tokens: bfloat16 [8, 128, 3200], P('dp', 'seq'), may hold values from -6 to 6
- proj_weight: bfloat16 [3200, 8192], P('dp', 'seq')
- text_hidden: bfloat16 [8, 512, 8192], P('dp', 'seq'), may hold values from -6 to 6
- cotangent: bfloat16 [8, 512, 8192], P('dp', 'seq'), may hold values from -1.1953125 to 1.1953125
- norm_gain: float32 [8192], replicated, may hold values from 0.25 to 1.75
- placeholders: int32 [8, 128], P('dp'), may hold values from 0 to 511, as said below
- bucket_levels: int32 [8, 4, 3200], P('dp', 'seq'), may hold values from 2 to 16
- row_draws: float32 [8, 4, 3200], P('dp', 'seq'), may hold values from 0 to 1
- column_draws: float32 [8, 8192], P('dp', 'seq'), may hold values from 0 to 1
Outputs:
- weight_grad: float32 [3200, 8192], P('dp', 'seq')
- gain_grad: float32 [8192], replicated
The draws below stay inside these ranges and needn't reach their ends.
Inputs may be any that keep to these rules, and one draw needn't show every extreme that they name: Each row is strictly increasing. Among the positions of one device's block of 128 positions stand at most 48 placeholders, and in every row some block holds exactly 48.
All inputs are finite; a program needn't handle non-finite values.
Results may differ from the reference program's by a relative error of at most 0.014.
Values may be sent and summed in bfloat16 or wider, within the bound.
No kernel may reach another device: no remote copies, remote signals or barrier semaphores. Data moves between devices by JAX's collectives and lax.ppermute only.
A program may use at most 64 MiB of HBM per device.

```python
import math
import jax
import jax.numpy as jnp
from jax import lax

VD = 3200
D = 8192
IMG_DEV = 32
TOK_DEV = 128
IMG = 128
TOKENS = 512
N_DP = 8
N_SEQ = 4


def draw_proj_weight(key, part):
    group_width = max(D // 64, 1)
    group_total = D // group_width
    first_key, second_key = jax.random.split(jax.random.fold_in(key, 11))
    logs = jax.random.uniform(second_key, (group_total,), jnp.float32, -1.15, 1.15)
    column_scale = jnp.repeat(jnp.exp(logs), group_width)
    base = jax.random.normal(first_key, (VD, D), jnp.float32)
    return (base * column_scale[None, :] / math.sqrt(VD)).astype(jnp.bfloat16)


def placeholder_list(key):
    owner_total = TOKENS // TOK_DEV
    half_extra = IMG_DEV // 2
    order_key, amount_key, choose_key = jax.random.split(key, 3)
    order = jax.random.permutation(order_key, owner_total)
    amounts = jax.random.randint(amount_key, (owner_total // 2,), 0, half_extra + 1)
    amounts = amounts.at[0].set(half_extra)
    paired = jnp.stack([amounts, -amounts], axis=1).reshape(-1)
    delta = jnp.zeros((owner_total,), jnp.int32).at[order].set(paired.astype(jnp.int32))
    counts = IMG_DEV + delta
    owner_keys = jax.random.split(choose_key, owner_total)
    ranking = jax.vmap(lambda one_key: jax.random.permutation(one_key, TOK_DEV))(owner_keys)
    chosen = (ranking < counts[:, None]).reshape(-1)
    sort_keys = jnp.where(chosen, 0, 1) * TOKENS + jnp.arange(TOKENS, dtype=jnp.int32)
    return jnp.argsort(sort_keys)[:IMG].astype(jnp.int32)


def draw_placeholders(key, part):
    replica_keys = jax.random.split(jax.random.fold_in(key, 23), N_DP)
    return jax.vmap(placeholder_list)(replica_keys)


def set_ends(array, rng, low, largest):
    index_at = [jax.random.randint(jax.random.fold_in(rng, axis), (), 0, length) for axis, length in enumerate(array.shape)]
    main_axis = array.shape.index(max(array.shape))
    beside = index_at[:main_axis] + [(index_at[main_axis] + 1) % array.shape[main_axis]] + index_at[main_axis + 1:]
    return array.at[tuple(index_at)].set(low).at[tuple(beside)].set(largest)


def strengthened(entries, rng, source, target, shards_of, factor):
    owner, partner = [(jnp.arange(entries.shape[position]) // (entries.shape[position] // shards_of)).reshape([-1 if axis == position else 1 for axis in range(entries.ndim)]) for position in (source, target)]
    chosen = jax.random.permutation(rng, shards_of)[partner]
    strong = (owner == chosen) | (owner == (partner + shards_of // 2) % shards_of)
    return jnp.where(strong, factor * entries, entries)


def block_levels(rng, extent, pieces, least, largest):
    loudness = 1.0
    for position, shards_of in pieces:
        draws = jax.random.uniform(jax.random.fold_in(jax.random.fold_in(rng, 6), position), (shards_of,), jnp.float32, least / len(pieces), largest / len(pieces))
        loudness = loudness * jnp.repeat(jnp.exp(draws), extent[position] // shards_of).reshape((-1,) + (1,) * (len(extent) - 1 - position))
    return loudness


def noise(rng, dims, spread, reach, pieces=(), kind=jnp.bfloat16):
    array = jax.random.normal(rng, dims, jnp.float32) * spread
    if len(pieces) > 0:
        array = block_levels(rng, dims, pieces, -0.22, 0.18) * array
    return jnp.clip(array, min=-reach, max=reach).astype(kind)


def bell_draw_with(own_key, dims, deviation, reach, shards, heavy, held_as=jnp.bfloat16):
    values = deviation * jax.random.normal(own_key, dims, jnp.float32)
    if shards:
        values = values * block_levels(own_key, dims, shards, -0.22, 0.18)
    return jnp.clip(strengthened(values, jax.random.fold_in(own_key, 3), *heavy), -reach, reach).astype(held_as)


def setup_inputs(seed: int = 0) -> dict:
    keys = jax.random.split(jax.random.key(seed), 10)
    return {
        "tile_tokens": bell_draw_with(keys[0], (N_DP, IMG, VD), 1.0, 6.0, ((0, 8), (1, 4)), (0, 2, 8, 2.0)),
        "proj_weight": draw_proj_weight(jax.random.fold_in(keys[9], 71), 0),
        "text_hidden": noise(keys[2], (N_DP, TOKENS, D), 1.0, 6.0, ((0, 8), (1, 4))),
        "cotangent": noise(keys[3], (N_DP, TOKENS, D), 0.2, 1.1953125, ((0, 8), (1, 4))),
        "norm_gain": jnp.clip(1.0 + 0.15 * jax.random.normal(keys[4], (D,), jnp.float32), 0.25, 1.75),
        "placeholders": draw_placeholders(jax.random.fold_in(keys[9], 71), 0),
        "bucket_levels": set_ends(jax.random.randint(keys[6], (N_DP, N_SEQ, VD), 2, 17), jax.random.fold_in(keys[6], 1), 2, 16).astype(jnp.int32),
        "row_draws": jnp.clip(1.0 * jax.random.uniform(keys[7], (N_DP, N_SEQ, VD), jnp.float32) ** block_levels(keys[7], (N_DP, N_SEQ, VD), ((0, 8), (1, 4)), -0.2, 0.2), 0.0, 1.0),
        "column_draws": jnp.clip(1.0 * jax.random.uniform(keys[8], (N_DP, D), jnp.float32) ** block_levels(keys[8], (N_DP, D), ((0, 8), (1, 4)), -0.2, 0.2), 0.0, 1.0),
    }


EPSILON = 1e-06

def quantize(gradient, levels_now, rows_now, columns_now):
    buckets = levels_now.shape[0]
    grouped = gradient.reshape(gradient.shape[0], buckets, -1)
    bucket_norm = jnp.sqrt(lax.optimization_barrier(jnp.sum(grouped * grouped, axis=2, keepdims=True)) + EPSILON)
    step_count = jnp.transpose(levels_now).astype(jnp.float32)[:, :, None]
    offset = 0.25 + 0.25 * (jnp.transpose(rows_now)[:, :, None] + columns_now.reshape(buckets, -1)[None, :, :])
    ratio = jnp.abs(grouped) / bucket_norm * step_count
    lower = jnp.floor(ratio)
    quantum = lower + jnp.clip(2.0 * (ratio - lower - offset) + 0.5, 0.0, 1.0)
    return (jnp.sign(grouped) * bucket_norm * quantum / step_count).reshape(gradient.shape)

def reference(tile_tokens, proj_weight, text_hidden, cotangent, norm_gain, placeholders, bucket_levels, row_draws, column_draws):

    def replica(running, inputs):
        weight_sum, gain_sum = running
        tile_rows, text_rows, cot_rows, places, levels_now, rows_now, columns_now = inputs
        embedded = jnp.dot(tile_rows, proj_weight, preferred_element_type=jnp.float32).astype(jnp.bfloat16)
        image_marks = jnp.zeros((TOKENS,), jnp.int32).at[places].set(1)
        image_ranks = jnp.clip(jnp.cumsum(image_marks) - image_marks, 0, IMG - 1).astype(jnp.int32)
        hidden = jnp.where(image_marks[:, None] == 1, jnp.take(embedded, image_ranks, axis=0), text_rows)
        hidden_f = hidden.astype(jnp.float32)
        inverse = lax.rsqrt(lax.optimization_barrier(jnp.mean(hidden_f * hidden_f, axis=1, keepdims=True)) + EPSILON)
        normed = hidden_f * inverse
        cot_float = cot_rows.astype(jnp.float32)
        grad_in = cot_float * norm_gain[None, :]
        hidden_grad = ((grad_in - normed * lax.optimization_barrier(jnp.mean(grad_in * normed, axis=1, keepdims=True))) * inverse).astype(jnp.bfloat16)
        emb_grad = jnp.take(hidden_grad, places, axis=0)
        gradient = lax.dot_general(tile_rows, emb_grad, (((0,), (0,)), ((), ())), preferred_element_type=jnp.float32)
        quantized = quantize(gradient, levels_now, rows_now, columns_now)
        rounded = lax.optimization_barrier(quantized.astype(jnp.bfloat16)).astype(jnp.float32)
        return ((weight_sum + rounded, gain_sum + lax.optimization_barrier(jnp.sum(cot_float * normed, axis=0))), None)
    initial = (jnp.zeros((VD, D), jnp.float32), jnp.zeros((D,), jnp.float32))
    inputs = (tile_tokens, text_hidden, cotangent, placeholders, bucket_levels, row_draws, column_draws)
    (weight_sum, gain_sum), unused = lax.scan(replica, initial, inputs)
    return (weight_sum / N_DP, gain_sum / N_DP)
```

```python
import functools

import jax
import jax.numpy as jnp
from jax import lax
from jax.experimental import pallas as pl
from jax.experimental.pallas import tpu as pltpu
from jax.sharding import PartitionSpec as P


IMG_MOST = 48
META_ROWS = 16
EXTRA_ROWS = 8
EPSILON = 1e-06
FLOAT = jnp.float32
HALF = jnp.bfloat16


def whole(*_):
    return pl.BlockSpec(memory_space=pltpu.VMEM)


def scalar():
    return pl.BlockSpec(memory_space=pltpu.SMEM)


def grant(mebibytes):
    return pltpu.CompilerParams(vmem_limit_bytes=mebibytes << 20)


def lanes(count):
    return -(-count // 128) * 128


def flip(value, bit):
    count = lax.axis_size("dp")
    return lax.ppermute(value, "dp", [(i, i ^ (1 << bit)) for i in range(count)])


def swap(value, step):
    count = lax.axis_size("seq")
    return lax.ppermute(value, "seq", [(i, i ^ step) for i in range(count)])


def pieces(value):
    high = lax.reduce_precision(value, 8, 7)
    rest = value - high
    mid = lax.reduce_precision(rest, 8, 7)
    return high, mid, rest - mid


def cast_pieces(value):
    high = value.astype(HALF).astype(FLOAT)
    rest = value - high
    mid = rest.astype(HALF).astype(FLOAT)
    return high, mid, rest - mid


def stacked_lines(values, lines, width):
    line = lax.broadcasted_iota(jnp.int32, (lines, width), 0)
    block = jnp.zeros((lines, width), FLOAT)
    for index, value in enumerate(values):
        block = jnp.where(line == index, value, block)
    return block


def pack_kernel(tile_ref, level_ref, draw_ref, out_ref):
    owners, _, width = out_ref.shape
    rows, full = tile_ref.shape
    terms = (level_ref[...].astype(FLOAT),) + cast_pieces(draw_ref[...])
    extra = stacked_lines(terms, META_ROWS, full).astype(HALF)
    for owner in range(owners):
        cut = slice(owner * width, (owner + 1) * width)
        out_ref[owner, :rows, :] = tile_ref[:, cut]
        out_ref[owner, rows:, :] = extra[:, cut]


def unpack_kernel(order, place_ref, in_ref, tile_ref, meta_ref, tile_scratch, meta_scratch):
    replicas, rows, width = in_ref.shape
    tokens = rows - META_ROWS
    kept = tile_ref.shape[0]
    tile_scratch[...] = jnp.zeros_like(tile_scratch)
    meta_scratch[...] = jnp.zeros_like(meta_scratch)
    for slot, relative in enumerate(order):
        block = in_ref[place_ref[0] ^ relative].astype(FLOAT)
        tile_scratch[slot * tokens : (slot + 1) * tokens, :width] = block[:tokens]
        meta = block[tokens:]
        meta_scratch[relative : relative + 1, :width] = meta[0:1]
        meta_scratch[replicas + relative : replicas + relative + 1, :width] = (
            meta[1:2] + meta[2:3] + meta[3:4]
        )
    tile_ref[...] = tile_scratch[...].T[:kept].astype(HALF)
    meta_ref[...] = meta_scratch[...].T[:kept]


def regroup_kernel(order, tokens, *refs):
    count = len(refs) - len(order)
    for slot, relative in enumerate(order):
        cut = slice(slot * tokens, (slot + 1) * tokens)
        refs[count + relative][...] = jnp.concatenate([ref[:, cut] for ref in refs[:count]], axis=1)


def text_kernel(place_ref, row_ref, column_ref, text_ref, cot_ref, out_ref):
    owners, _, columns = out_ref.shape
    rows, full = text_ref.shape
    count = row_ref.shape[1]
    mine = place_ref[0]
    base = mine * rows
    position = lax.broadcasted_iota(jnp.int32, (rows, count), 0)
    hits = (row_ref[...] - base == position).astype(FLOAT)
    is_text = 1.0 - jnp.max(hits, axis=1, keepdims=True)
    start = jnp.sum((row_ref[...] < base).astype(jnp.int32), axis=1, keepdims=True)
    token = lax.broadcasted_iota(jnp.int32, (IMG_MOST, count), 1)
    slot = lax.broadcasted_iota(jnp.int32, (IMG_MOST, count), 0)
    chosen = (token - start == slot).astype(HALF)
    spread = (
        column_ref[...] - base == lax.broadcasted_iota(jnp.int32, (count, rows), 1)
    ).astype(HALF)
    select = jnp.dot(chosen, spread, preferred_element_type=FLOAT).astype(HALF)
    total = jnp.zeros((rows, 1), FLOAT)
    for owner in range(owners):
        text = text_ref[:, owner * columns : (owner + 1) * columns].astype(FLOAT)
        total = total + jnp.sum(text * text, axis=1, keepdims=True)
    inverse = lax.rsqrt(total / full + EPSILON) * is_text
    for step in range(owners):
        owner = mine ^ step
        cut = pl.ds(pl.multiple_of(owner * columns, columns), columns)
        cot = cot_ref[:, cut]
        terms = cot.astype(FLOAT) * text_ref[:, cut].astype(FLOAT) * inverse
        part = jnp.sum(terms, axis=0, keepdims=True)
        out_ref[step, :IMG_MOST, :] = jnp.dot(
            select, cot, preferred_element_type=FLOAT
        ).astype(HALF)
        out_ref[step, IMG_MOST:, :] = stacked_lines(
            cast_pieces(part), EXTRA_ROWS, columns
        ).astype(HALF)


def quantize_kernel(slots, replicas, adds, *refs):
    count = len(slots)
    tile_refs = refs[:count]
    meta_ref = refs[count]
    loads = refs[count + 1 : 2 * count + 1]
    total_ref = refs[2 * count + 1] if adds else None
    out_ref, gradient, half_draw, row_half, lever, weight = refs[-6:]
    rows, columns = out_ref.shape
    tokens = tile_refs[0].shape[1]
    groups = rows // 8
    strips = [slice(at, at + 128) for at in range(0, columns, 128)]
    unroll = 5 if groups % 5 == 0 else 2
    for index, relative in enumerate(slots):
        load = loads[index]
        gradient[...] = jnp.dot(
            tile_refs[index][...], load[:tokens, :], preferred_element_type=FLOAT
        )
        extra = load[tokens:, :].astype(FLOAT)
        draw = 0.5 * (extra[3:4] + extra[4:5] + extra[5:6])
        half_draw[...] = jnp.broadcast_to(draw, (8, columns))

        def sum_group(step, carry):
            cut = pl.ds(pl.multiple_of(step * 8, 8), 8)
            parts = [gradient[cut, strip] for strip in strips]
            parts = [part * part for part in parts]
            while len(parts) > 1:
                parts = [a + b for a, b in zip(parts[::2], parts[1::2])] + parts[len(parts) & ~1 :]
            lever[cut, :] = parts[0]
            return carry

        lax.fori_loop(0, groups, sum_group, 0, unroll=unroll)
        norm = jnp.sqrt(jnp.sum(lever[...], axis=1, keepdims=True) + EPSILON)
        levels = meta_ref[:, relative : relative + 1]
        row_draw = meta_ref[:, replicas + relative : replicas + relative + 1]
        row_half[...] = jnp.broadcast_to(0.5 * row_draw, lever.shape)
        lever[...] = jnp.broadcast_to(levels / norm, lever.shape)
        weight[...] = jnp.broadcast_to(norm / (levels * replicas), lever.shape)

        def group(step, carry):
            cut = pl.ds(pl.multiple_of(step * 8, 8), 8)
            factor = lever[cut, :]
            scale = weight[cut, :]
            opposite = -scale
            row_shift = row_half[cut, :]
            for strip in strips:
                entry = gradient[cut, strip]
                ratio = jnp.abs(entry) * factor
                lower = jnp.floor(ratio)
                part = ratio - lower
                shift = half_draw[:, strip] + row_shift
                quantum = lower + jnp.clip(part + part - shift, 0.0, 1.0)
                term = jnp.where(entry < 0.0, opposite, scale) * quantum
                if index > 0:
                    term = term + out_ref[cut, strip]
                elif adds:
                    term = term + total_ref[cut, strip]
                out_ref[cut, strip] = term
            return carry

        lax.fori_loop(0, groups, group, 0, unroll=unroll)


def quantized_sum(tiles, meta, loads, slots, replicas, total, last):
    rows, _ = tiles[0].shape
    columns = loads[0].shape[1]
    adds = total is not None
    return pl.pallas_call(
        functools.partial(quantize_kernel, slots, replicas, adds),
        in_specs=[whole()] * (2 * len(slots) + 1 + adds),
        out_specs=whole(),
        out_shape=jax.ShapeDtypeStruct((rows, columns), FLOAT),
        scratch_shapes=[
            pltpu.VMEM((rows, columns), FLOAT),
            pltpu.VMEM((8, columns), FLOAT),
            pltpu.VMEM((rows, 128), FLOAT),
            pltpu.VMEM((rows, 128), FLOAT),
            pltpu.VMEM((rows, 128), FLOAT),
        ],
        input_output_aliases={2 * len(slots) + 1: 0} if adds and not last else {},
        compiler_params=grant(12),
        cost_estimate=pl.CostEstimate(
            flops=len(slots) * rows * columns * 1200, bytes_accessed=0, transcendentals=0
        ),
        name="quantized_sum",
    )(*[tiles[slot] for slot in slots], meta, *loads, *([total] if adds else []))


def stack_blocks(stats, step):
    return jnp.stack([stats[:, at ^ step] for at in range(stats.shape[1])], axis=1)


def half_of(value, bit, taken):
    shape = value.shape
    high = shape[0] // (2 * bit)
    cut = value.reshape((high, 2, bit) + shape[1:])[:, taken]
    return cut.reshape((high * bit,) + shape[1:])


def on_device(
    tile_tokens,
    proj_weight,
    text_hidden,
    cotangent,
    norm_gain,
    placeholders,
    bucket_levels,
    row_draws,
    column_draws,
):
    seq_count = lax.axis_size("seq")
    seq_index = lax.axis_index("seq")
    replicas = lax.axis_size("dp")
    replica = lax.axis_index("dp")
    levels_of_bits = replicas.bit_length() - 1
    assert replicas == 1 << levels_of_bits
    places = placeholders[0]
    image_total = places.shape[0]
    tok_rows, model_width = text_hidden.shape[1:]
    tile_rows, _ = tile_tokens.shape[1:]
    width, columns = proj_weight.shape
    padded = -(-width // 16) * 16
    order = tuple(range(0, replicas, 2)) + tuple(range(1, replicas, 2))
    here = replica.astype(jnp.int32).reshape(1)
    there = seq_index.astype(jnp.int32).reshape(1)

    packed = pl.pallas_call(
        pack_kernel,
        in_specs=[whole()] * 3,
        out_specs=whole(),
        out_shape=jax.ShapeDtypeStruct((replicas, tile_rows + META_ROWS, width), HALF),
        compiler_params=grant(4),
        name="pack",
    )(tile_tokens[0], bucket_levels[0], row_draws[0])
    exchanged = lax.all_to_all(packed, "dp", 0, 0, tiled=True)
    own_tile, meta = pl.pallas_call(
        functools.partial(unpack_kernel, order),
        in_specs=[scalar(), whole()],
        out_specs=[whole(), whole()],
        out_shape=[
            jax.ShapeDtypeStruct((padded, replicas * tile_rows), HALF),
            jax.ShapeDtypeStruct((padded, lanes(2 * replicas)), FLOAT),
        ],
        scratch_shapes=[
            pltpu.VMEM((lanes(replicas * tile_rows), lanes(width)), FLOAT),
            pltpu.VMEM((lanes(2 * replicas), lanes(width)), FLOAT),
        ],
        compiler_params=grant(8),
        name="unpack",
    )(here, exchanged)
    tile_blocks = [own_tile]
    for step in range(1, seq_count):
        tile_blocks.append(swap(own_tile, step))

    outgoing = pl.pallas_call(
        text_kernel,
        in_specs=[scalar()] + [whole()] * 4,
        out_specs=whole(),
        out_shape=jax.ShapeDtypeStruct((seq_count, IMG_MOST + EXTRA_ROWS, columns), HALF),
        cost_estimate=pl.CostEstimate(
            flops=tok_rows * model_width * 4000, bytes_accessed=0, transcendentals=0
        ),
        compiler_params=grant(16),
        name="text_part",
    )(there, placeholders, places.reshape(image_total, 1), text_hidden[0], cotangent[0])
    outgoing, last = lax.optimization_barrier((outgoing, tile_blocks[-1]))
    tile_blocks[-1] = last
    returned = [outgoing[0]]
    for step in range(1, seq_count):
        returned.append(swap(outgoing[step], step))

    weight = jnp.pad(proj_weight, ((0, padded - width), (0, 0)))
    even = (replicas // 2) * tile_rows
    split = seq_count // 2
    bit_orders = (
        tuple(range(1, levels_of_bits)),
        tuple(reversed(range(1, levels_of_bits))),
    )
    parts = (tile_blocks[:split], tile_blocks[split:])
    embedded_parts = []
    for group, bits in zip(parts, bit_orders):

        def product(cut, kind):
            left = jnp.concatenate([block[:, cut] for block in group], axis=1)
            out = lax.dot_general(
                left, weight, (((0,), (0,)), ((), ())), preferred_element_type=FLOAT
            ).astype(kind)
            out = out.reshape(len(group), replicas // 2, tile_rows, columns)
            return jnp.transpose(out, (1, 0, 2, 3))

        sent = product(slice(even, 2 * even), HALF)
        held = product(slice(0, even), FLOAT)
        arrived = flip(sent, 0)
        remaining = list(range(1, levels_of_bits))
        for bit in bits:
            stride = 1 << remaining.index(bit)
            remaining.remove(bit)
            held = held + arrived.astype(FLOAT)
            sent = half_of(held, stride, 1).astype(HALF)
            held = half_of(held, stride, 0)
            arrived = flip(sent, bit)
        held = held + arrived.astype(FLOAT)
        embedded_parts.append(held.reshape(-1, columns))
    emb_float = jnp.concatenate(embedded_parts, axis=0).astype(HALF).astype(FLOAT)

    tokens = jnp.arange(image_total, dtype=jnp.int32)
    absolute = ((tokens // tile_rows) ^ there) * tile_rows + tokens % tile_rows
    sources = jnp.arange(seq_count, dtype=jnp.int32) ^ there
    starts = jnp.sum((places[None, :] < (sources * tok_rows)[:, None]).astype(jnp.int32), axis=1)
    wanted = (absolute[:, None] - starts[None, :])[:, :, None]
    match = (wanted == jnp.arange(IMG_MOST, dtype=jnp.int32)[None, None, :]).astype(HALF)
    arrived = jnp.concatenate([block[:IMG_MOST] for block in returned], axis=0)
    image_cot = jnp.dot(
        match.reshape(image_total, seq_count * IMG_MOST), arrived, preferred_element_type=FLOAT
    )
    text_part = sum(
        jnp.sum(block[IMG_MOST : IMG_MOST + 3].astype(FLOAT), axis=0) for block in returned
    )

    column_gain = lax.dynamic_slice_in_dim(norm_gain, seq_index * columns, columns)
    grad_in = image_cot * column_gain[None, :]
    stats = jnp.stack(
        [jnp.sum(emb_float * emb_float, axis=1), jnp.sum(grad_in * emb_float, axis=1)]
    ).reshape(2, seq_count, tile_rows)
    for_all = stats
    for step in range(1, seq_count):
        for_all = for_all + swap(stack_blocks(stats, step), step)
    squares, mixed = for_all.reshape(2, image_total)
    inverse = lax.rsqrt(squares / model_width + EPSILON)[:, None]
    normed = emb_float * inverse
    emb_grad = ((grad_in - normed * (mixed[:, None] * inverse / model_width)) * inverse).astype(HALF)
    gain_part = text_part + jnp.sum(image_cot * normed, axis=0)
    extra = jnp.stack(
        pieces(gain_part)
        + pieces(column_draws[0])
        + (jnp.zeros_like(gain_part),) * (EXTRA_ROWS - 6)
    ).astype(HALF)
    own_load = jnp.concatenate([emb_grad, extra], axis=0)

    tiles = pl.pallas_call(
        functools.partial(regroup_kernel, order, tile_rows),
        in_specs=[whole()] * seq_count,
        out_specs=[whole()] * replicas,
        out_shape=[jax.ShapeDtypeStruct((padded, image_total), HALF)] * replicas,
        cost_estimate=pl.CostEstimate(
            flops=replicas * padded * image_total * 2000, bytes_accessed=0, transcendentals=0
        ),
        compiler_params=grant(8),
        name="regroup",
    )(*tile_blocks)

    loads = {0: own_load}
    if levels_of_bits == 3:
        loads[1] = flip(own_load, 0)
        loads[2] = flip(own_load, 1)
        loads[4] = flip(own_load, 2)
        is_low = (replica & 1) == 0
        passed = jnp.where(is_low, loads[2], loads[4])
        pairs = [(i, i ^ (4 if i % 2 == 0 else 2)) for i in range(replicas)]
        loads[6] = lax.ppermute(passed, "dp", pairs)
        for slot in (2, 4, 6):
            loads[slot + 1] = flip(loads[slot], 0)
        batches = ((0, 1), (2, 4), (3, 5), (6, 7))
    else:
        for bit in tuple(range(1, levels_of_bits)) + (0,):
            loads.update({slot ^ (1 << bit): flip(load, bit) for slot, load in list(loads.items())})
        batches = tuple((slot, slot + 1) for slot in range(0, replicas, 2))
    total = None
    for slots in batches:
      total = quantized_sum(tiles, meta, [loads[slot] for slot in slots], slots, replicas, total, slots == batches[-1])
    gain_rows = sum(
        jnp.sum(load[image_total : image_total + 3].astype(FLOAT), axis=0) for load in loads.values()
    )
    gain_rows = (gain_rows / replicas).reshape(8, columns // 8)
    gains = jnp.stack([gain_rows] + [swap(gain_rows, step) for step in range(1, seq_count)])
    gain_total = jnp.take(gains, sources, axis=0)
    return total[:width], gain_total.reshape(model_width)


def solution(mesh):
    return jax.shard_map(
        on_device,
        mesh=mesh,
        in_specs=(
            P("dp", "seq", None),
            P("dp", "seq"),
            P("dp", "seq", None),
            P("dp", "seq", None),
            P(),
            P("dp", None),
            P("dp", "seq", None),
            P("dp", "seq", None),
            P("dp", "seq"),
        ),
        out_specs=(P("dp", "seq"), P()),
        check_vma=False,
    )
```

```python
import functools

import jax
import jax.numpy as jnp
from jax import lax
from jax.experimental import pallas as pl
from jax.experimental.pallas import tpu as pltpu
from jax.sharding import PartitionSpec as P


IMG_MOST = 48
META_ROWS = 16
EXTRA_ROWS = 8
EPSILON = 1e-06
FLOAT = jnp.float32
HALF = jnp.bfloat16


def whole(*_):
    return pl.BlockSpec(memory_space=pltpu.VMEM)


def scalar():
    return pl.BlockSpec(memory_space=pltpu.SMEM)


def grant(mebibytes):
    return pltpu.CompilerParams(vmem_limit_bytes=mebibytes << 20)


def lanes(count):
    return -(-count // 128) * 128


def flip(value, bit):
    count = lax.axis_size("dp")
    return lax.ppermute(value, "dp", [(i, i ^ (1 << bit)) for i in range(count)])


def exchanged_label(label, levels):
    upper = levels - 1
    if upper % 2:
        return label
    half = upper // 2
    mask = (1 << half) - 1
    first, second = (label >> 1) & mask, (label >> (1 + half)) & mask
    return (label & 1) | (second << 1) | (first << (1 + half))


def flip_label(value, bit):
    count = lax.axis_size("dp")
    levels = count.bit_length() - 1
    odd = exchanged_label(1 << bit, levels)
    return lax.ppermute(
        value, "dp", [(i, i ^ (odd if i % 2 else 1 << bit)) for i in range(count)]
    )


def swap(value, step):
    count = lax.axis_size("seq")
    return lax.ppermute(value, "seq", [(i, i ^ step) for i in range(count)])


def pieces(value):
    high = lax.reduce_precision(value, 8, 7)
    rest = value - high
    mid = lax.reduce_precision(rest, 8, 7)
    return high, mid, rest - mid


def cast_pieces(value):
    high = value.astype(HALF).astype(FLOAT)
    rest = value - high
    mid = rest.astype(HALF).astype(FLOAT)
    return high, mid, rest - mid


def stacked_lines(values, lines, width):
    line = lax.broadcasted_iota(jnp.int32, (lines, width), 0)
    block = jnp.zeros((lines, width), FLOAT)
    for index, value in enumerate(values):
        block = jnp.where(line == index, value, block)
    return block


def pack_kernel(tile_ref, level_ref, draw_ref, out_ref):
    owners, _, width = out_ref.shape
    rows, full = tile_ref.shape
    terms = (level_ref[...].astype(FLOAT),) + cast_pieces(draw_ref[...])
    extra = stacked_lines(terms, META_ROWS, full).astype(HALF)
    for owner in range(owners):
        cut = slice(owner * width, (owner + 1) * width)
        out_ref[owner, :rows, :] = tile_ref[:, cut]
        out_ref[owner, rows:, :] = extra[:, cut]


def unpack_kernel(order, place_ref, in_ref, tile_ref, meta_ref, tile_scratch, meta_scratch):
    replicas, rows, width = in_ref.shape
    tokens = rows - META_ROWS
    kept = tile_ref.shape[0]
    levels = replicas.bit_length() - 1
    core = place_ref[0] & 1
    tile_scratch[...] = jnp.zeros_like(tile_scratch)
    meta_scratch[...] = jnp.zeros_like(meta_scratch)
    for slot, relative in enumerate(order):
        other = exchanged_label(relative, levels)
        block = in_ref[place_ref[0] ^ (relative + core * (other - relative))].astype(FLOAT)
        tile_scratch[slot * tokens : (slot + 1) * tokens, :width] = block[:tokens]
        meta = block[tokens:]
        meta_scratch[relative : relative + 1, :width] = meta[0:1]
        meta_scratch[replicas + relative : replicas + relative + 1, :width] = (
            meta[1:2] + meta[2:3] + meta[3:4]
        )
    tile_ref[...] = tile_scratch[...].T[:kept].astype(HALF)
    meta_ref[...] = meta_scratch[...].T[:kept]


def regroup_kernel(order, tokens, *refs):
    out_ref = refs[-1]
    total = tokens * (len(refs) - 1)
    for slot, relative in enumerate(order):
        cut = slice(slot * tokens, (slot + 1) * tokens)
        out_ref[:, relative * total : (relative + 1) * total] = jnp.concatenate(
            [ref[:, cut] for ref in refs[:-1]], axis=1
        )


def text_kernel(place_ref, row_ref, column_ref, text_ref, cot_ref, out_ref):
    owners, _, columns = out_ref.shape
    rows, full = text_ref.shape
    count = row_ref.shape[1]
    mine = place_ref[0]
    base = mine * rows
    position = lax.broadcasted_iota(jnp.int32, (rows, count), 0)
    hits = (row_ref[...] - base == position).astype(FLOAT)
    is_text = 1.0 - jnp.max(hits, axis=1, keepdims=True)
    start = jnp.sum((row_ref[...] < base).astype(jnp.int32), axis=1, keepdims=True)
    token = lax.broadcasted_iota(jnp.int32, (IMG_MOST, count), 1)
    slot = lax.broadcasted_iota(jnp.int32, (IMG_MOST, count), 0)
    chosen = (token - start == slot).astype(HALF)
    spread = (
        column_ref[...] - base == lax.broadcasted_iota(jnp.int32, (count, rows), 1)
    ).astype(HALF)
    select = jnp.dot(chosen, spread, preferred_element_type=FLOAT).astype(HALF)
    total = jnp.zeros((rows, 1), FLOAT)
    for owner in range(owners):
        text = text_ref[:, owner * columns : (owner + 1) * columns].astype(FLOAT)
        total = total + jnp.sum(text * text, axis=1, keepdims=True)
    inverse = lax.rsqrt(total / full + EPSILON) * is_text
    for step in range(owners):
        owner = mine ^ step
        cut = pl.ds(pl.multiple_of(owner * columns, columns), columns)
        cot = cot_ref[:, cut]
        terms = cot.astype(FLOAT) * text_ref[:, cut].astype(FLOAT) * inverse
        part = jnp.sum(terms, axis=0, keepdims=True)
        out_ref[step, :IMG_MOST, :] = jnp.dot(
            select, cot, preferred_element_type=FLOAT
        ).astype(HALF)
        out_ref[step, IMG_MOST:, :] = stacked_lines(
            cast_pieces(part), EXTRA_ROWS, columns
        ).astype(HALF)


def quantize_kernel(slots, replicas, adds, *refs):
    count = len(slots)
    tile_ref, meta_ref = refs[:2]
    loads = refs[2 : count + 2]
    total_ref = refs[count + 2] if adds else None
    out_ref, gradient, half_draw, row_half, lever, weight = refs[-6:]
    rows, columns = out_ref.shape
    tokens = tile_ref.shape[1] // replicas
    groups = rows // 8
    strips = [slice(at, at + 128) for at in range(0, columns, 128)]
    unroll = 5 if groups % 5 == 0 else 2
    for index, relative in enumerate(slots):
        load = loads[index]
        gradient[...] = jnp.dot(
            tile_ref[:, relative * tokens : (relative + 1) * tokens],
            load[:tokens, :],
            preferred_element_type=FLOAT,
        )
        extra = load[tokens:, :].astype(FLOAT)
        draw = 0.5 * (extra[3:4] + extra[4:5] + extra[5:6])
        half_draw[...] = jnp.broadcast_to(draw, (8, columns))

        def sum_group(step, carry):
            cut = pl.ds(pl.multiple_of(step * 8, 8), 8)
            parts = [gradient[cut, strip] for strip in strips]
            parts = [part * part for part in parts]
            while len(parts) > 1:
                parts = [a + b for a, b in zip(parts[::2], parts[1::2])] + parts[len(parts) & ~1 :]
            lever[cut, :] = parts[0]
            return carry

        lax.fori_loop(0, groups, sum_group, 0, unroll=unroll)
        norm = jnp.sqrt(jnp.sum(lever[...], axis=1, keepdims=True) + EPSILON)
        levels = meta_ref[:, relative : relative + 1]
        row_draw = meta_ref[:, replicas + relative : replicas + relative + 1]
        row_half[...] = jnp.broadcast_to(0.5 * row_draw, lever.shape)
        lever[...] = jnp.broadcast_to(levels / norm, lever.shape)
        weight[...] = jnp.broadcast_to(norm / (levels * replicas), lever.shape)

        def group(step, carry):
            cut = pl.ds(pl.multiple_of(step * 8, 8), 8)
            factor = lever[cut, :]
            scale = weight[cut, :]
            opposite = -scale
            row_shift = row_half[cut, :]
            for strip in strips:
                entry = gradient[cut, strip]
                ratio = jnp.abs(entry) * factor
                lower = jnp.floor(ratio)
                part = ratio - lower
                shift = half_draw[:, strip] + row_shift
                quantum = lower + jnp.clip(part + part - shift, 0.0, 1.0)
                term = jnp.where(entry < 0.0, opposite, scale) * quantum
                if index > 0:
                    term = term + out_ref[cut, strip]
                elif adds:
                    term = term + total_ref[cut, strip]
                out_ref[cut, strip] = term
            return carry

        lax.fori_loop(0, groups, group, 0, unroll=unroll)


def gain_kernel(replicas, *refs):
    tokens = refs[0].shape[0] - EXTRA_ROWS
    total = jnp.zeros(refs[-1].shape, FLOAT)
    for ref in refs[:-1]:
        extra = ref[tokens:, :].astype(FLOAT)
        total = total + (extra[0:1] + extra[1:2] + extra[2:3])
    refs[-1][...] = total / replicas


def quantized_sum(tiles, meta, loads, slots, replicas, total):
    rows = tiles.shape[0]
    columns = loads[0].shape[1]
    adds = total is not None
    return pl.pallas_call(
        functools.partial(quantize_kernel, slots, replicas, adds),
        in_specs=[whole()] * (len(slots) + 2 + adds),
        out_specs=whole(),
        out_shape=jax.ShapeDtypeStruct((rows, columns), FLOAT),
        scratch_shapes=[
            pltpu.VMEM((rows, columns), FLOAT),
            pltpu.VMEM((8, columns), FLOAT),
            pltpu.VMEM((rows, 128), FLOAT),
            pltpu.VMEM((rows, 128), FLOAT),
            pltpu.VMEM((rows, 128), FLOAT),
        ],
        compiler_params=grant(12),
        cost_estimate=pl.CostEstimate(
            flops=len(slots) * rows * columns * 1200, bytes_accessed=0, transcendentals=0
        ),
        name="quantized_sum",
    )(tiles, meta, *loads, *([total] if adds else []))


def stack_blocks(stats, step):
    return jnp.stack([stats[:, at ^ step] for at in range(stats.shape[1])], axis=1)


def half_of(value, bit, taken):
    shape = value.shape
    high = shape[0] // (2 * bit)
    cut = value.reshape((high, 2, bit) + shape[1:])[:, taken]
    return cut.reshape((high * bit,) + shape[1:])


def on_device(
    tile_tokens,
    proj_weight,
    text_hidden,
    cotangent,
    norm_gain,
    placeholders,
    bucket_levels,
    row_draws,
    column_draws,
):
    seq_count = lax.axis_size("seq")
    seq_index = lax.axis_index("seq")
    replicas = lax.axis_size("dp")
    replica = lax.axis_index("dp")
    levels_of_bits = replicas.bit_length() - 1
    assert replicas == 1 << levels_of_bits
    places = placeholders[0]
    image_total = places.shape[0]
    tok_rows, model_width = text_hidden.shape[1:]
    tile_rows, _ = tile_tokens.shape[1:]
    width, columns = proj_weight.shape
    padded = -(-width // 16) * 16
    kept_labels = tuple(range(0, replicas, 2))
    order = kept_labels + tuple(exchanged_label(label, levels_of_bits) ^ 1 for label in kept_labels)
    here = replica.astype(jnp.int32).reshape(1)
    there = seq_index.astype(jnp.int32).reshape(1)

    packed = pl.pallas_call(
        pack_kernel,
        in_specs=[whole()] * 3,
        out_specs=whole(),
        out_shape=jax.ShapeDtypeStruct((replicas, tile_rows + META_ROWS, width), HALF),
        compiler_params=grant(4),
        name="pack",
    )(tile_tokens[0], bucket_levels[0], row_draws[0])
    exchanged = lax.all_to_all(packed, "dp", 0, 0, tiled=True)
    own_tile, meta = pl.pallas_call(
        functools.partial(unpack_kernel, order),
        in_specs=[scalar(), whole()],
        out_specs=[whole(), whole()],
        out_shape=[
            jax.ShapeDtypeStruct((padded, replicas * tile_rows), HALF),
            jax.ShapeDtypeStruct((padded, lanes(2 * replicas)), FLOAT),
        ],
        scratch_shapes=[
            pltpu.VMEM((lanes(replicas * tile_rows), lanes(width)), FLOAT),
            pltpu.VMEM((lanes(2 * replicas), lanes(width)), FLOAT),
        ],
        compiler_params=grant(8),
        name="unpack",
    )(here, exchanged)
    tile_blocks = [own_tile]
    for step in range(1, seq_count):
        tile_blocks.append(swap(own_tile, step))

    outgoing = pl.pallas_call(
        text_kernel,
        in_specs=[scalar()] + [whole()] * 4,
        out_specs=whole(),
        out_shape=jax.ShapeDtypeStruct((seq_count, IMG_MOST + EXTRA_ROWS, columns), HALF),
        cost_estimate=pl.CostEstimate(
            flops=tok_rows * model_width * 4000, bytes_accessed=0, transcendentals=0
        ),
        compiler_params=grant(16),
        name="text_part",
    )(there, placeholders, places.reshape(image_total, 1), text_hidden[0], cotangent[0])

    weight = jnp.pad(proj_weight, ((0, padded - width), (0, 0)))
    even = (replicas // 2) * tile_rows
    split = seq_count // 2
    parts = [tile_blocks[:split]] + [[block] for block in tile_blocks[split:]]
    embedded_parts = []
    for part, group in enumerate(parts):

        def product(cut, kind):
            left = jnp.concatenate([block[:, cut] for block in group], axis=1)
            out = lax.dot_general(
                left, weight, (((0,), (0,)), ((), ())), preferred_element_type=FLOAT
            ).astype(kind)
            out = out.reshape(len(group), replicas // 2, tile_rows, columns)
            return jnp.transpose(out, (1, 0, 2, 3))

        sent = product(slice(even, 2 * even), HALF)
        held = product(slice(0, even), FLOAT)
        if part == 0:
            outgoing, sent = lax.optimization_barrier((outgoing, sent))
            returned = [outgoing[0]]
            for step in range(1, seq_count):
                returned.append(swap(outgoing[step], step))
        arrived = flip(sent, 0)
        remaining = list(range(1, levels_of_bits))
        for bit in range(1, levels_of_bits):
            stride = 1 << remaining.index(bit)
            remaining.remove(bit)
            held = held + arrived.astype(FLOAT)
            sent = half_of(held, stride, 1).astype(HALF)
            held = half_of(held, stride, 0)
            arrived = flip_label(sent, bit)
        held = held + arrived.astype(FLOAT)
        embedded_parts.append(held.reshape(-1, columns))
    emb_float = jnp.concatenate(embedded_parts, axis=0).astype(HALF).astype(FLOAT)

    tokens = jnp.arange(image_total, dtype=jnp.int32)
    absolute = ((tokens // tile_rows) ^ there) * tile_rows + tokens % tile_rows
    sources = jnp.arange(seq_count, dtype=jnp.int32) ^ there
    starts = jnp.sum((places[None, :] < (sources * tok_rows)[:, None]).astype(jnp.int32), axis=1)
    wanted = (absolute[:, None] - starts[None, :])[:, :, None]
    match = (wanted == jnp.arange(IMG_MOST, dtype=jnp.int32)[None, None, :]).astype(HALF)
    arrived = jnp.concatenate([block[:IMG_MOST] for block in returned], axis=0)
    image_cot = jnp.dot(
        match.reshape(image_total, seq_count * IMG_MOST), arrived, preferred_element_type=FLOAT
    )
    text_part = sum(
        jnp.sum(block[IMG_MOST : IMG_MOST + 3].astype(FLOAT), axis=0) for block in returned
    )

    column_gain = lax.dynamic_slice_in_dim(norm_gain, seq_index * columns, columns)
    grad_in = image_cot * column_gain[None, :]
    stats = jnp.stack(
        [jnp.sum(emb_float * emb_float, axis=1), jnp.sum(grad_in * emb_float, axis=1)]
    ).reshape(2, seq_count, tile_rows)
    for_all = stats
    for step in range(1, seq_count):
        for_all = for_all + swap(stack_blocks(stats, step), step)
    squares, mixed = for_all.reshape(2, image_total)
    inverse = lax.rsqrt(squares / model_width + EPSILON)[:, None]
    normed = emb_float * inverse
    emb_grad = ((grad_in - normed * (mixed[:, None] * inverse / model_width)) * inverse).astype(HALF)
    gain_part = text_part + jnp.sum(image_cot * normed, axis=0)
    extra = jnp.stack(
        pieces(gain_part)
        + pieces(column_draws[0])
        + (jnp.zeros_like(gain_part),) * (EXTRA_ROWS - 6)
    ).astype(HALF)
    own_load = jnp.concatenate([emb_grad, extra], axis=0)

    tiles = pl.pallas_call(
        functools.partial(regroup_kernel, order, tile_rows),
        in_specs=[whole()] * seq_count,
        out_specs=whole(),
        out_shape=jax.ShapeDtypeStruct((padded, replicas * image_total), HALF),
        cost_estimate=pl.CostEstimate(
            flops=replicas * padded * image_total * 2000, bytes_accessed=0, transcendentals=0
        ),
        compiler_params=grant(8),
        name="regroup",
    )(*tile_blocks)

    loads = {0: own_load}
    if levels_of_bits == 3:
        loads[1] = flip(own_load, 0)
        loads[2] = flip_label(own_load, 1)
        loads[5] = flip(loads[2], 0)
        loads[4] = flip_label(own_load, 2)
        loads[3] = flip(loads[4], 0)
        loads[6] = flip_label(loads[2], 2)
        loads[7] = flip(loads[6], 0)
        batches = ((0, 1), (2, 5), (4,), (3, 6), (7,))
    else:
        for bit in range(1, levels_of_bits):
            for slot, load in list(loads.items()):
                loads[slot ^ (1 << bit)] = flip_label(load, bit)
        for slot, load in list(loads.items()):
            loads[exchanged_label(slot, levels_of_bits) ^ 1] = flip(load, 0)
        batches = tuple((slot, slot + 1) for slot in range(0, replicas, 2))
    gain_row = pl.pallas_call(
        functools.partial(gain_kernel, replicas),
        in_specs=[whole()] * replicas,
        out_specs=whole(),
        out_shape=jax.ShapeDtypeStruct((1, columns), FLOAT),
        compiler_params=grant(12),
        name="gain",
    )(*[loads[slot] for slot in range(replicas)])
    gains = [gain_row]
    for step in range(1, seq_count):
        gains.append(swap(gain_row, step))
    total = None
    for slots in batches:
        total = quantized_sum(tiles, meta, [loads[slot] for slot in slots], slots, replicas, total)
    gain_total = jnp.take(jnp.concatenate(gains, axis=0), sources, axis=0)
    return total[:width], gain_total.reshape(model_width)


def solution(mesh):
    return jax.shard_map(
        on_device,
        mesh=mesh,
        in_specs=(
            P("dp", "seq", None),
            P("dp", "seq"),
            P("dp", "seq", None),
            P("dp", "seq", None),
            P(),
            P("dp", None),
            P("dp", "seq", None),
            P("dp", "seq", None),
            P("dp", "seq"),
        ),
        out_specs=(P("dp", "seq"), P()),
        check_vma=False,
    )
```

```python
import functools

import jax
import jax.numpy as jnp
from jax import lax
from jax.experimental import pallas as pl
from jax.experimental.pallas import tpu as pltpu
from jax.sharding import PartitionSpec as P


IMG_MOST = 48
META_ROWS = 16
EXTRA_ROWS = 8
EPSILON = 1e-06
FLOAT = jnp.float32
HALF = jnp.bfloat16


def whole(*_):
    return pl.BlockSpec(memory_space=pltpu.VMEM)


def anywhere():
    return pl.BlockSpec(memory_space=pltpu.HBM)


def scalar():
    return pl.BlockSpec(memory_space=pltpu.SMEM)


def grant(mebibytes):
    return pltpu.CompilerParams(vmem_limit_bytes=mebibytes << 20)


def lanes(count):
    return -(-count // 128) * 128


def flip(value, bit):
    count = lax.axis_size("dp")
    return lax.ppermute(value, "dp", [(i, i ^ (1 << bit)) for i in range(count)])


def exchanged_label(label, levels):
    upper = levels - 1
    if upper % 2:
        return label
    half = upper // 2
    mask = (1 << half) - 1
    first, second = (label >> 1) & mask, (label >> (1 + half)) & mask
    return (label & 1) | (second << 1) | (first << (1 + half))


def flip_label(value, bit):
    count = lax.axis_size("dp")
    levels = count.bit_length() - 1
    odd = exchanged_label(1 << bit, levels)
    return lax.ppermute(
        value, "dp", [(i, i ^ (odd if i % 2 else 1 << bit)) for i in range(count)]
    )


def flip_far(value):
    count = lax.axis_size("dp")
    return lax.ppermute(value, "dp", [(i, i ^ 6) for i in range(count)])


def swap(value, step):
    count = lax.axis_size("seq")
    return lax.ppermute(value, "seq", [(i, i ^ step) for i in range(count)])


def cast_pieces(value):
    high = value.astype(HALF).astype(FLOAT)
    rest = value - high
    mid = rest.astype(HALF).astype(FLOAT)
    return high, mid, rest - mid


def stacked_lines(values, lines, width):
    line = lax.broadcasted_iota(jnp.int32, (lines, width), 0)
    block = jnp.zeros((lines, width), FLOAT)
    for index, value in enumerate(values):
        block = jnp.where(line == index, value, block)
    return block


def fetch(pairs, sems):
    copies = [
        pltpu.make_async_copy(source, target, sems.at[index])
        for index, (source, target) in enumerate(pairs)
    ]
    for copy in copies:
        copy.start()
    return copies


def pack_kernel(tile_hbm, level_hbm, draw_hbm, out_ref, tile_ref, level_ref, draw_ref, sems):
    pairs = ((tile_hbm, tile_ref), (level_hbm, level_ref), (draw_hbm, draw_ref))
    for copy in fetch(pairs, sems):
        copy.wait()
    owners, _, width = out_ref.shape
    rows, full = tile_ref.shape
    terms = (level_ref[...].astype(FLOAT),) + cast_pieces(draw_ref[...])
    extra = stacked_lines(terms, META_ROWS, full).astype(HALF)
    for owner in range(owners):
        cut = slice(owner * width, (owner + 1) * width)
        out_ref[owner, :rows, :] = tile_ref[:, cut]
        out_ref[owner, rows:, :] = extra[:, cut]


def unpack_kernel(order, place_ref, in_ref, tile_ref, meta_ref, tile_scratch, meta_scratch):
    replicas, rows, width = in_ref.shape
    tokens = rows - META_ROWS
    kept = tile_ref.shape[0]
    levels = replicas.bit_length() - 1
    core = place_ref[0] & 1
    tile_scratch[...] = jnp.zeros_like(tile_scratch)
    meta_scratch[...] = jnp.zeros_like(meta_scratch)
    for slot, relative in enumerate(order):
        other = exchanged_label(relative, levels)
        block = in_ref[place_ref[0] ^ (relative + core * (other - relative))].astype(FLOAT)
        tile_scratch[slot * tokens : (slot + 1) * tokens, :width] = block[:tokens]
        meta = block[tokens:]
        meta_scratch[relative : relative + 1, :width] = meta[0:1]
        meta_scratch[replicas + relative : replicas + relative + 1, :width] = (
            meta[1:2] + meta[2:3] + meta[3:4]
        )
    tile_ref[...] = tile_scratch[...].T[:kept].astype(HALF)
    meta_ref[...] = meta_scratch[...].T[:kept]


def regroup_kernel(order, tokens, *refs):
    out_ref = refs[-1]
    total = tokens * (len(refs) - 1)
    for slot, relative in enumerate(order):
        cut = slice(slot * tokens, (slot + 1) * tokens)
        out_ref[:, relative * total : (relative + 1) * total] = jnp.concatenate(
            [ref[:, cut] for ref in refs[:-1]], axis=1
        )


def text_kernel(
    place_ref, row_ref, column_ref, text_hbm, cot_hbm, out_ref, part_ref, text_ref, cot_ref, sems
):
    owners, _, columns = out_ref.shape
    rows, full = text_hbm.shape
    cuts = [slice(owner * columns, (owner + 1) * columns) for owner in range(owners)]
    pairs = [(text_hbm.at[:, cut], text_ref.at[:, cut]) for cut in cuts]
    pairs += [(cot_hbm.at[:, cut], cot_ref.at[:, cut]) for cut in cuts]
    copies = fetch(pairs, sems)
    count = row_ref.shape[1]
    mine = place_ref[0]
    base = mine * rows
    position = lax.broadcasted_iota(jnp.int32, (rows, count), 0)
    hits = (row_ref[...] - base == position).astype(FLOAT)
    is_text = 1.0 - jnp.max(hits, axis=1, keepdims=True)
    start = jnp.sum((row_ref[...] < base).astype(jnp.int32), axis=1, keepdims=True)
    token = lax.broadcasted_iota(jnp.int32, (IMG_MOST, count), 1)
    slot = lax.broadcasted_iota(jnp.int32, (IMG_MOST, count), 0)
    chosen = (token - start == slot).astype(HALF)
    spread = (
        column_ref[...] - base == lax.broadcasted_iota(jnp.int32, (count, rows), 1)
    ).astype(HALF)
    select = jnp.dot(chosen, spread, preferred_element_type=FLOAT).astype(HALF)
    total = jnp.zeros((rows, 1), FLOAT)
    for owner in range(owners):
        copies[owner].wait()
        text = text_ref[:, cuts[owner]].astype(FLOAT)
        total = total + jnp.sum(text * text, axis=1, keepdims=True)
    inverse = lax.rsqrt(total / full + EPSILON) * is_text
    for copy in copies[owners:]:
        copy.wait()
    for step in range(owners):
        owner = mine ^ step
        cut = pl.ds(pl.multiple_of(owner * columns, columns), columns)
        cot = cot_ref[:, cut]
        terms = cot.astype(FLOAT) * text_ref[:, cut].astype(FLOAT) * inverse
        part_ref[step] = jnp.sum(terms, axis=0, keepdims=True)
        out_ref[step] = jnp.dot(select, cot, preferred_element_type=FLOAT).astype(HALF)


def quantize_kernel(slots, replicas, adds, *refs):
    count = len(slots)
    tile_ref, meta_ref = refs[:2]
    loads = refs[2 : count + 2]
    total_ref = refs[count + 2] if adds else None
    out_ref, gradient, half_draw, row_half, lever, weight = refs[-6:]
    rows, columns = out_ref.shape
    tokens = tile_ref.shape[1] // replicas
    groups = rows // 8
    strips = [slice(at, at + 128) for at in range(0, columns, 128)]
    unroll = 5 if groups % 5 == 0 else 2
    for index, relative in enumerate(slots):
        load = loads[index]
        gradient[...] = jnp.dot(
            tile_ref[:, relative * tokens : (relative + 1) * tokens],
            load[:tokens, :],
            preferred_element_type=FLOAT,
        )
        extra = load[tokens:, :].astype(FLOAT)
        draw = 0.5 * (extra[3:4] + extra[4:5] + extra[5:6])
        half_draw[...] = jnp.broadcast_to(draw, (8, columns))

        def sum_group(step, carry):
            cut = pl.ds(pl.multiple_of(step * 8, 8), 8)
            parts = [gradient[cut, strip] for strip in strips]
            parts = [part * part for part in parts]
            while len(parts) > 1:
                parts = [a + b for a, b in zip(parts[::2], parts[1::2])] + parts[len(parts) & ~1 :]
            lever[cut, :] = parts[0]
            return carry

        lax.fori_loop(0, groups, sum_group, 0, unroll=unroll)
        norm = jnp.sqrt(jnp.sum(lever[...], axis=1, keepdims=True) + EPSILON)
        levels = meta_ref[:, relative : relative + 1]
        row_draw = meta_ref[:, replicas + relative : replicas + relative + 1]
        row_half[...] = jnp.broadcast_to(0.5 * row_draw, lever.shape)
        lever[...] = jnp.broadcast_to(levels / norm, lever.shape)
        weight[...] = jnp.broadcast_to(norm / (levels * replicas), lever.shape)

        def group(step, carry):
            cut = pl.ds(pl.multiple_of(step * 8, 8), 8)
            factor = lever[cut, :]
            scale = weight[cut, :]
            opposite = -scale
            row_shift = row_half[cut, :]
            for strip in strips:
                entry = gradient[cut, strip]
                ratio = jnp.abs(entry) * factor
                lower = jnp.floor(ratio)
                part = ratio - lower
                shift = half_draw[:, strip] + row_shift
                quantum = lower + jnp.clip(part + part - shift, 0.0, 1.0)
                term = jnp.where(entry < 0.0, opposite, scale) * quantum
                if index > 0:
                    term = term + out_ref[cut, strip]
                elif adds:
                    term = term + total_ref[cut, strip]
                out_ref[cut, strip] = term
            return carry

        lax.fori_loop(0, groups, group, 0, unroll=unroll)


def own_gain(gain_ref, mine, columns):
    return gain_ref[:, pl.ds(pl.multiple_of(mine * columns, columns), columns)]


def middle_kernel(sizes, owners, owner_rows, place_ref, row_ref, gain_ref, part_ref, *refs):
    sums = []
    for size in sizes:
        total = refs[0][...]
        for ref in refs[1:size]:
            total = total + ref[...].astype(FLOAT)
        sums.append(total)
        refs = refs[size:]
    blocks, emb_ref, cot_ref = refs[:owners], refs[owners], refs[owners + 1]
    stats = refs[owners + 2 :]
    mine = place_ref[0]
    tokens, columns = emb_ref.shape
    block_rows = tokens // owners
    shift = block_rows.bit_length() - 1
    emb = jnp.concatenate(sums, axis=0).astype(HALF)
    emb_ref[...] = emb
    emb = emb.astype(FLOAT)
    line = lax.broadcasted_iota(jnp.int32, (tokens, IMG_MOST), 0)
    slot = lax.broadcasted_iota(jnp.int32, (tokens, IMG_MOST), 1)
    absolute = ((line >> shift) ^ mine) * block_rows + (line & (block_rows - 1))
    cot = jnp.zeros((tokens, columns), FLOAT)
    for step in range(owners):
        first = (mine ^ step) * owner_rows
        start = jnp.sum((row_ref[...] < first).astype(jnp.int32), axis=1, keepdims=True)
        match = (absolute - start == slot).astype(HALF)
        cot = cot + jnp.dot(match, blocks[step][...], preferred_element_type=FLOAT)
    cot_ref[...] = cot.astype(HALF)
    grad = cot * own_gain(gain_ref, mine, columns)
    sums = (
        jnp.sum(emb * emb, axis=1, keepdims=True),
        jnp.sum(grad * emb, axis=1, keepdims=True),
    )
    width = lanes(2 * owners)
    lane = lax.broadcasted_iota(jnp.int32, (tokens, width), 1)
    table = jnp.zeros((tokens, width), FLOAT)
    for step in range(owners):
        for which, column in enumerate(sums):
            moved = jnp.concatenate(
                [
                    column[(at ^ step) * block_rows : ((at ^ step) + 1) * block_rows]
                    for at in range(owners)
                ],
                axis=0,
            )
            table = jnp.where(lane == 2 * step + which, moved, table)
    turned = table.T
    for step in range(owners):
        stats[step][...] = jnp.concatenate(
            [turned[2 * step : 2 * step + 1], turned[2 * step + 1 : 2 * step + 2], part_ref[step]],
            axis=1,
        )


def finish_kernel(owners, full, place_ref, gain_ref, emb_ref, cot_ref, draw_ref, *refs):
    stats, out_ref, scratch = refs[:owners], refs[-2], refs[-1]
    tokens, columns = emb_ref.shape
    scratch[...] = jnp.zeros_like(scratch)
    total = stats[0][...]
    for ref in stats[1:]:
        total = total + ref[...]
    scratch[0:1, :] = total[:, :tokens]
    scratch[1:2, :] = total[:, tokens : 2 * tokens]
    turned = scratch[...].T
    inverse = lax.rsqrt(turned[:, 0:1] / full + EPSILON)
    cot = cot_ref[...].astype(FLOAT)
    normed = emb_ref[...].astype(FLOAT) * inverse
    grad = cot * own_gain(gain_ref, place_ref[0], columns)
    out_ref[:tokens, :] = (
        (grad - normed * (turned[:, 1:2] * inverse / full)) * inverse
    ).astype(HALF)
    part = total[:, 2 * tokens :] + jnp.sum(cot * normed, axis=0, keepdims=True)
    terms = cast_pieces(part) + cast_pieces(draw_ref[...])
    out_ref[tokens:, :] = stacked_lines(terms, EXTRA_ROWS, columns).astype(HALF)


def gain_kernel(replicas, *refs):
    tokens = refs[0].shape[0] - EXTRA_ROWS
    total = jnp.zeros(refs[-1].shape, FLOAT)
    for ref in refs[:-1]:
        extra = ref[tokens:, :].astype(FLOAT)
        total = total + (extra[0:1] + extra[1:2] + extra[2:3])
    refs[-1][...] = total / replicas


def quantized_sum(tiles, meta, loads, slots, replicas, total):
    rows = tiles.shape[0]
    columns = loads[0].shape[1]
    adds = total is not None
    return pl.pallas_call(
        functools.partial(quantize_kernel, slots, replicas, adds),
        in_specs=[whole()] * (len(slots) + 2 + adds),
        out_specs=whole(),
        out_shape=jax.ShapeDtypeStruct((rows, columns), FLOAT),
        scratch_shapes=[
            pltpu.VMEM((rows, columns), FLOAT),
            pltpu.VMEM((8, columns), FLOAT),
            pltpu.VMEM((rows, 128), FLOAT),
            pltpu.VMEM((rows, 128), FLOAT),
            pltpu.VMEM((rows, 128), FLOAT),
        ],
        compiler_params=grant(12),
        cost_estimate=pl.CostEstimate(
            flops=len(slots) * rows * columns * 1200, bytes_accessed=0, transcendentals=0
        ),
        name="quantized_sum",
    )(tiles, meta, *loads, *([total] if adds else []))


def half_of(value, bit, taken):
    shape = value.shape
    high = shape[0] // (2 * bit)
    cut = value.reshape((high, 2, bit) + shape[1:])[:, taken]
    return cut.reshape((high * bit,) + shape[1:])


def on_device(
    tile_tokens,
    proj_weight,
    text_hidden,
    cotangent,
    norm_gain,
    placeholders,
    bucket_levels,
    row_draws,
    column_draws,
):
    seq_count = lax.axis_size("seq")
    seq_index = lax.axis_index("seq")
    replicas = lax.axis_size("dp")
    replica = lax.axis_index("dp")
    levels_of_bits = replicas.bit_length() - 1
    assert replicas == 1 << levels_of_bits
    places = placeholders[0]
    image_total = places.shape[0]
    tok_rows, model_width = text_hidden.shape[1:]
    tile_rows, vision = tile_tokens.shape[1:]
    width, columns = proj_weight.shape
    padded = -(-width // 16) * 16
    kept_labels = tuple(range(0, replicas, 2))
    order = kept_labels + tuple(exchanged_label(label, levels_of_bits) ^ 1 for label in kept_labels)
    here = replica.astype(jnp.int32).reshape(1)
    there = seq_index.astype(jnp.int32).reshape(1)

    packed = pl.pallas_call(
        pack_kernel,
        in_specs=[anywhere()] * 3,
        out_specs=whole(),
        scratch_shapes=[
            pltpu.VMEM((tile_rows, vision), HALF),
            pltpu.VMEM((1, vision), jnp.int32),
            pltpu.VMEM((1, vision), FLOAT),
            pltpu.SemaphoreType.DMA((3,)),
        ],
        out_shape=jax.ShapeDtypeStruct((replicas, tile_rows + META_ROWS, width), HALF),
        compiler_params=grant(60),
        name="pack",
    )(tile_tokens[0], bucket_levels[0], row_draws[0])
    exchanged = lax.all_to_all(packed, "dp", 0, 0, tiled=True)
    own_tile, meta = pl.pallas_call(
        functools.partial(unpack_kernel, order),
        in_specs=[scalar(), whole()],
        out_specs=[whole(), whole()],
        out_shape=[
            jax.ShapeDtypeStruct((padded, replicas * tile_rows), HALF),
            jax.ShapeDtypeStruct((padded, lanes(2 * replicas)), FLOAT),
        ],
        scratch_shapes=[
            pltpu.VMEM((lanes(replicas * tile_rows), lanes(width)), FLOAT),
            pltpu.VMEM((lanes(2 * replicas), lanes(width)), FLOAT),
        ],
        compiler_params=grant(8),
        name="unpack",
    )(here, exchanged)
    tile_blocks = [own_tile]
    for step in range(1, seq_count):
        low = step & -step
        tile_blocks.append(swap(tile_blocks[step ^ low], low))

    outgoing, text_parts = pl.pallas_call(
        text_kernel,
        in_specs=[scalar()] + [whole()] * 2 + [anywhere()] * 2,
        out_specs=[whole()] * 2,
        scratch_shapes=[
            pltpu.VMEM((tok_rows, model_width), HALF),
            pltpu.VMEM((tok_rows, model_width), HALF),
            pltpu.SemaphoreType.DMA((2 * seq_count,)),
        ],
        out_shape=[
            jax.ShapeDtypeStruct((seq_count, IMG_MOST, columns), HALF),
            jax.ShapeDtypeStruct((seq_count, 1, columns), FLOAT),
        ],
        cost_estimate=pl.CostEstimate(
            flops=tok_rows * model_width * 4000, bytes_accessed=0, transcendentals=0
        ),
        compiler_params=grant(60),
        name="text_part",
    )(there, placeholders, places.reshape(image_total, 1), text_hidden[0], cotangent[0])

    weight = jnp.pad(proj_weight, ((0, padded - width), (0, 0)))
    even = (replicas // 2) * tile_rows
    split = seq_count // 2
    parts = [tile_blocks[:split]] + [[block] for block in tile_blocks[split:]]
    sizes, summands = [], []
    for part, group in enumerate(parts):

        def product(cut, kind):
            left = jnp.concatenate([block[:, cut] for block in group], axis=1)
            out = lax.dot_general(
                left, weight, (((0,), (0,)), ((), ())), preferred_element_type=FLOAT
            ).astype(kind)
            out = out.reshape(len(group), replicas // 2, tile_rows, columns)
            return jnp.transpose(out, (1, 0, 2, 3))

        sent = product(slice(even, 2 * even), HALF)
        held = product(slice(0, even), FLOAT)
        if part == 0:
            outgoing, sent = lax.optimization_barrier((outgoing, sent))
            returned = [outgoing[0]]
            for step in range(1, seq_count):
                returned.append(swap(outgoing[step], step))
        arrived = flip(sent, 0)
        held = held + arrived.astype(FLOAT)
        if levels_of_bits == 3 and part == len(parts) - 1:
            sums = [held[0]]
            for place in (1, 2, 3):
                sent = held[place].astype(HALF)
                sums.append(
                    flip_label(sent, place) if place < 3 else flip_far(sent)
                )
        else:
            for bit in range(1, levels_of_bits):
                sent = half_of(held, 1, 1).astype(HALF)
                held = half_of(held, 1, 0)
                arrived = flip_label(sent, bit)
                if bit < levels_of_bits - 1:
                    held = held + arrived.astype(FLOAT)
            sums = [held, arrived]
        sizes.append(len(sums))
        summands += [value.reshape(-1, columns) for value in sums]
    tokens_of = (image_total, columns)
    middle = pl.pallas_call(
        functools.partial(middle_kernel, tuple(sizes), seq_count, tok_rows),
        in_specs=[scalar()] + [whole()] * (3 + len(summands) + seq_count),
        out_specs=[whole()] * (2 + seq_count),
        out_shape=[
            jax.ShapeDtypeStruct(tokens_of, HALF),
            jax.ShapeDtypeStruct(tokens_of, HALF),
        ]
        + [jax.ShapeDtypeStruct((1, 2 * image_total + columns), FLOAT)] * seq_count,
        compiler_params=grant(16),
        name="middle",
    )(there, placeholders, norm_gain.reshape(1, -1), text_parts, *summands, *returned)
    embedded, image_cot = middle[:2]
    stats = [middle[2]]
    for step in range(1, seq_count):
        stats.append(swap(middle[2 + step], step))
    own_load = pl.pallas_call(
        functools.partial(finish_kernel, seq_count, model_width),
        in_specs=[scalar()] + [whole()] * (4 + seq_count),
        out_specs=whole(),
        out_shape=jax.ShapeDtypeStruct((image_total + EXTRA_ROWS, columns), HALF),
        scratch_shapes=[pltpu.VMEM((128, image_total), FLOAT)],
        compiler_params=grant(12),
        name="finish",
    )(there, norm_gain.reshape(1, -1), embedded, image_cot, column_draws, *stats)

    tiles = pl.pallas_call(
        functools.partial(regroup_kernel, order, tile_rows),
        in_specs=[whole()] * seq_count,
        out_specs=whole(),
        out_shape=jax.ShapeDtypeStruct((padded, replicas * image_total), HALF),
        cost_estimate=pl.CostEstimate(
            flops=replicas * padded * image_total * 2000, bytes_accessed=0, transcendentals=0
        ),
        compiler_params=grant(8),
        name="regroup",
    )(*tile_blocks)

    loads = {0: own_load}
    if levels_of_bits == 3:
        loads[1] = flip(own_load, 0)
        loads[2] = flip_label(own_load, 1)
        loads[5] = flip(loads[2], 0)
        loads[4] = flip_label(own_load, 2)
        loads[3] = flip(loads[4], 0)
        loads[6] = flip_label(loads[2], 2)
        loads[7] = flip(loads[6], 0)
        batches = ((0, 1), (2, 5), (4,), (3,), (6,), (7,))
    else:
        for bit in range(1, levels_of_bits):
            for slot, load in list(loads.items()):
                loads[slot ^ (1 << bit)] = flip_label(load, bit)
        for slot, load in list(loads.items()):
            loads[exchanged_label(slot, levels_of_bits) ^ 1] = flip(load, 0)
        batches = tuple((slot, slot + 1) for slot in range(0, replicas, 2))
    gain_row = pl.pallas_call(
        functools.partial(gain_kernel, replicas),
        in_specs=[whole()] * replicas,
        out_specs=whole(),
        out_shape=jax.ShapeDtypeStruct((1, columns), FLOAT),
        compiler_params=grant(12),
        name="gain",
    )(*[loads[slot] for slot in range(replicas)])
    gains = [gain_row]
    for step in range(1, seq_count):
        gains.append(swap(gain_row, step))
    total = None
    for slots in batches:
        total = quantized_sum(tiles, meta, [loads[slot] for slot in slots], slots, replicas, total)
    sources = jnp.arange(seq_count, dtype=jnp.int32) ^ there
    gain_total = jnp.take(jnp.concatenate(gains, axis=0), sources, axis=0)
    return total[:width], gain_total.reshape(model_width)


def solution(mesh):
    return jax.shard_map(
        on_device,
        mesh=mesh,
        in_specs=(
            P("dp", "seq", None),
            P("dp", "seq"),
            P("dp", "seq", None),
            P("dp", "seq", None),
            P(),
            P("dp", None),
            P("dp", "seq", None),
            P("dp", "seq", None),
            P("dp", "seq"),
        ),
        out_specs=(P("dp", "seq"), P()),
        check_vma=False,
    )
```

```python
import functools

import jax
import jax.numpy as jnp
from jax import lax
from jax.experimental import pallas as pl
from jax.experimental.pallas import tpu as pltpu
from jax.sharding import PartitionSpec as P


IMG_MOST = 48
META_ROWS = 16
EXTRA_ROWS = 8
EPSILON = 1e-06
FLOAT = jnp.float32
HALF = jnp.bfloat16


def whole(*_):
    return pl.BlockSpec(memory_space=pltpu.VMEM)


def anywhere():
    return pl.BlockSpec(memory_space=pltpu.HBM)


def scalar():
    return pl.BlockSpec(memory_space=pltpu.SMEM)


def grant(mebibytes):
    return pltpu.CompilerParams(vmem_limit_bytes=mebibytes << 20)


def lanes(count):
    return -(-count // 128) * 128


def flip(value, bit):
    count = lax.axis_size("dp")
    return lax.ppermute(value, "dp", [(i, i ^ (1 << bit)) for i in range(count)])


def exchanged_label(label, levels):
    upper = levels - 1
    if upper % 2:
        return label
    half = upper // 2
    mask = (1 << half) - 1
    first, second = (label >> 1) & mask, (label >> (1 + half)) & mask
    return (label & 1) | (second << 1) | (first << (1 + half))


def flip_label(value, bit):
    count = lax.axis_size("dp")
    levels = count.bit_length() - 1
    odd = exchanged_label(1 << bit, levels)
    return lax.ppermute(
        value, "dp", [(i, i ^ (odd if i % 2 else 1 << bit)) for i in range(count)]
    )


def flip_far(value):
    count = lax.axis_size("dp")
    return lax.ppermute(value, "dp", [(i, i ^ 6) for i in range(count)])


def swap(value, step):
    count = lax.axis_size("seq")
    return lax.ppermute(value, "seq", [(i, i ^ step) for i in range(count)])


def cast_pieces(value):
    high = value.astype(HALF).astype(FLOAT)
    rest = value - high
    mid = rest.astype(HALF).astype(FLOAT)
    return high, mid, rest - mid


def stacked_lines(values, lines, width):
    line = lax.broadcasted_iota(jnp.int32, (lines, width), 0)
    block = jnp.zeros((lines, width), FLOAT)
    for index, value in enumerate(values):
        block = jnp.where(line == index, value, block)
    return block


def fetch(pairs, sems):
    copies = [
        pltpu.make_async_copy(source, target, sems.at[index])
        for index, (source, target) in enumerate(pairs)
    ]
    for copy in copies:
        copy.start()
    return copies


def pack_kernel(tile_hbm, level_hbm, draw_hbm, out_ref, tile_ref, level_ref, draw_ref, sems):
    pairs = ((tile_hbm, tile_ref), (level_hbm, level_ref), (draw_hbm, draw_ref))
    for copy in fetch(pairs, sems):
        copy.wait()
    owners, _, width = out_ref.shape
    rows, full = tile_ref.shape
    terms = (level_ref[...].astype(FLOAT),) + cast_pieces(draw_ref[...])
    extra = stacked_lines(terms, META_ROWS, full).astype(HALF)
    for owner in range(owners):
        cut = slice(owner * width, (owner + 1) * width)
        out_ref[owner, :rows, :] = tile_ref[:, cut]
        out_ref[owner, rows:, :] = extra[:, cut]


def unpack_kernel(order, place_ref, in_ref, tile_ref, meta_ref, tile_scratch, meta_scratch):
    replicas, rows, width = in_ref.shape
    tokens = rows - META_ROWS
    kept = tile_ref.shape[0]
    levels = replicas.bit_length() - 1
    core = place_ref[0] & 1
    tile_scratch[...] = jnp.zeros_like(tile_scratch)
    meta_scratch[...] = jnp.zeros_like(meta_scratch)
    for slot, relative in enumerate(order):
        other = exchanged_label(relative, levels)
        block = in_ref[place_ref[0] ^ (relative + core * (other - relative))].astype(FLOAT)
        tile_scratch[slot * tokens : (slot + 1) * tokens, :width] = block[:tokens]
        meta = block[tokens:]
        meta_scratch[relative : relative + 1, :width] = meta[0:1]
        meta_scratch[replicas + relative : replicas + relative + 1, :width] = (
            meta[1:2] + meta[2:3] + meta[3:4]
        )
    tile_ref[...] = tile_scratch[...].T[:kept].astype(HALF)
    meta_ref[...] = meta_scratch[...].T[:kept]


def regroup_kernel(order, tokens, *refs):
    out_ref = refs[-1]
    total = tokens * (len(refs) - 1)
    for slot, relative in enumerate(order):
        cut = slice(slot * tokens, (slot + 1) * tokens)
        out_ref[:, relative * total : (relative + 1) * total] = jnp.concatenate(
            [ref[:, cut] for ref in refs[:-1]], axis=1
        )


def text_kernel(
    place_ref, row_ref, column_ref, text_hbm, cot_hbm, out_ref, part_ref, text_ref, cot_ref, sems
):
    owners, _, columns = out_ref.shape
    rows, full = text_hbm.shape
    cuts = [slice(owner * columns, (owner + 1) * columns) for owner in range(owners)]
    pairs = [(text_hbm.at[:, cut], text_ref.at[:, cut]) for cut in cuts]
    pairs += [(cot_hbm.at[:, cut], cot_ref.at[:, cut]) for cut in cuts]
    copies = fetch(pairs, sems)
    count = row_ref.shape[1]
    mine = place_ref[0]
    base = mine * rows
    position = lax.broadcasted_iota(jnp.int32, (rows, count), 0)
    hits = (row_ref[...] - base == position).astype(FLOAT)
    is_text = 1.0 - jnp.max(hits, axis=1, keepdims=True)
    start = jnp.sum((row_ref[...] < base).astype(jnp.int32), axis=1, keepdims=True)
    token = lax.broadcasted_iota(jnp.int32, (IMG_MOST, count), 1)
    slot = lax.broadcasted_iota(jnp.int32, (IMG_MOST, count), 0)
    chosen = (token - start == slot).astype(HALF)
    spread = (
        column_ref[...] - base == lax.broadcasted_iota(jnp.int32, (count, rows), 1)
    ).astype(HALF)
    select = jnp.dot(chosen, spread, preferred_element_type=FLOAT).astype(HALF)
    total = jnp.zeros((rows, 1), FLOAT)
    for owner in range(owners):
        copies[owner].wait()
        text = text_ref[:, cuts[owner]].astype(FLOAT)
        total = total + jnp.sum(text * text, axis=1, keepdims=True)
    inverse = lax.rsqrt(total / full + EPSILON) * is_text
    for copy in copies[owners:]:
        copy.wait()
    for step in range(owners):
        owner = mine ^ step
        cut = pl.ds(pl.multiple_of(owner * columns, columns), columns)
        cot = cot_ref[:, cut]
        terms = cot.astype(FLOAT) * text_ref[:, cut].astype(FLOAT) * inverse
        part_ref[step] = jnp.sum(terms, axis=0, keepdims=True)
        out_ref[step] = jnp.dot(select, cot, preferred_element_type=FLOAT).astype(HALF)


def quantize_kernel(slots, replicas, adds, chunks, *refs):
    count = len(slots)
    tile_ref, meta_ref = refs[:2]
    loads = refs[2 : count + 2]
    total_ref = refs[count + 2] if adds else None
    out_ref, gradient, half_draw, row_half, lever, weight = refs[count + 2 + adds :][:6]
    if chunks > 1:
        result, sems = out_ref, refs[-1]
        out_ref = refs[-2]
    rows, columns = out_ref.shape
    tokens = tile_ref.shape[1] // replicas
    groups = rows // 8
    strips = [slice(at, at + 128) for at in range(0, columns, 128)]
    unroll = 5 if groups % 5 == 0 else 2
    for index, relative in enumerate(slots):
        load = loads[index]
        gradient[...] = jnp.dot(
            tile_ref[:, relative * tokens : (relative + 1) * tokens],
            load[:tokens, :],
            preferred_element_type=FLOAT,
        )
        extra = load[tokens:, :].astype(FLOAT)
        draw = 0.5 * (extra[3:4] + extra[4:5] + extra[5:6])
        half_draw[...] = jnp.broadcast_to(draw, (8, columns))

        def sum_group(step, carry):
            cut = pl.ds(pl.multiple_of(step * 8, 8), 8)
            parts = [gradient[cut, strip] for strip in strips]
            parts = [part * part for part in parts]
            while len(parts) > 1:
                parts = [a + b for a, b in zip(parts[::2], parts[1::2])] + parts[len(parts) & ~1 :]
            lever[cut, :] = parts[0]
            return carry

        lax.fori_loop(0, groups, sum_group, 0, unroll=unroll)
        norm = jnp.sqrt(jnp.sum(lever[...], axis=1, keepdims=True) + EPSILON)
        levels = meta_ref[:, relative : relative + 1]
        row_draw = meta_ref[:, replicas + relative : replicas + relative + 1]
        row_half[...] = jnp.broadcast_to(0.5 * row_draw, lever.shape)
        lever[...] = jnp.broadcast_to(levels / norm, lever.shape)
        weight[...] = jnp.broadcast_to(norm / (levels * replicas), lever.shape)

        def group(step, carry):
            cut = pl.ds(pl.multiple_of(step * 8, 8), 8)
            factor = lever[cut, :]
            scale = weight[cut, :]
            opposite = -scale
            row_shift = row_half[cut, :]
            for strip in strips:
                entry = gradient[cut, strip]
                ratio = jnp.abs(entry) * factor
                lower = jnp.floor(ratio)
                part = ratio - lower
                shift = half_draw[:, strip] + row_shift
                quantum = lower + jnp.clip(part + part - shift, 0.0, 1.0)
                term = jnp.where(entry < 0.0, opposite, scale) * quantum
                if index > 0:
                    term = term + out_ref[cut, strip]
                elif adds:
                    term = term + total_ref[cut, strip]
                out_ref[cut, strip] = term
            return carry

        if chunks == 1 or index < count - 1:
            lax.fori_loop(0, groups, group, 0, unroll=unroll)
            continue
        copies = []
        for chunk in range(chunks):
            size = groups // chunks
            lax.fori_loop(chunk * size, (chunk + 1) * size, group, 0, unroll=unroll)
            cut = pl.ds(chunk * size * 8, size * 8)
            copy = pltpu.make_async_copy(out_ref.at[cut, :], result.at[cut, :], sems.at[chunk])
            copy.start()
            copies.append(copy)
        for copy in copies:
            copy.wait()


def own_gain(gain_ref, mine, columns):
    return gain_ref[:, pl.ds(pl.multiple_of(mine * columns, columns), columns)]


def middle_kernel(sizes, owners, owner_rows, place_ref, row_ref, gain_ref, part_ref, *refs):
    sums = []
    for size in sizes:
        total = refs[0][...]
        for ref in refs[1:size]:
            total = total + ref[...].astype(FLOAT)
        sums.append(total)
        refs = refs[size:]
    blocks, emb_ref, cot_ref = refs[:owners], refs[owners], refs[owners + 1]
    stats = refs[owners + 2 :]
    mine = place_ref[0]
    tokens, columns = emb_ref.shape
    block_rows = tokens // owners
    shift = block_rows.bit_length() - 1
    emb = jnp.concatenate(sums, axis=0).astype(HALF)
    emb_ref[...] = emb
    emb = emb.astype(FLOAT)
    line = lax.broadcasted_iota(jnp.int32, (tokens, IMG_MOST), 0)
    slot = lax.broadcasted_iota(jnp.int32, (tokens, IMG_MOST), 1)
    absolute = ((line >> shift) ^ mine) * block_rows + (line & (block_rows - 1))
    cot = jnp.zeros((tokens, columns), FLOAT)
    for step in range(owners):
        first = (mine ^ step) * owner_rows
        start = jnp.sum((row_ref[...] < first).astype(jnp.int32), axis=1, keepdims=True)
        match = (absolute - start == slot).astype(HALF)
        cot = cot + jnp.dot(match, blocks[step][...], preferred_element_type=FLOAT)
    cot_ref[...] = cot.astype(HALF)
    grad = cot * own_gain(gain_ref, mine, columns)
    sums = (
        jnp.sum(emb * emb, axis=1, keepdims=True),
        jnp.sum(grad * emb, axis=1, keepdims=True),
    )
    width = lanes(2 * owners)
    lane = lax.broadcasted_iota(jnp.int32, (tokens, width), 1)
    table = jnp.zeros((tokens, width), FLOAT)
    for step in range(owners):
        for which, column in enumerate(sums):
            moved = jnp.concatenate(
                [
                    column[(at ^ step) * block_rows : ((at ^ step) + 1) * block_rows]
                    for at in range(owners)
                ],
                axis=0,
            )
            table = jnp.where(lane == 2 * step + which, moved, table)
    turned = table.T
    for step in range(owners):
        stats[step][...] = jnp.concatenate(
            [turned[2 * step : 2 * step + 1], turned[2 * step + 1 : 2 * step + 2], part_ref[step]],
            axis=1,
        )


def finish_kernel(owners, full, place_ref, gain_ref, emb_ref, cot_ref, draw_ref, *refs):
    stats, out_ref, scratch = refs[:owners], refs[-2], refs[-1]
    tokens, columns = emb_ref.shape
    scratch[...] = jnp.zeros_like(scratch)
    total = stats[0][...]
    for ref in stats[1:]:
        total = total + ref[...]
    scratch[0:1, :] = total[:, :tokens]
    scratch[1:2, :] = total[:, tokens : 2 * tokens]
    turned = scratch[...].T
    inverse = lax.rsqrt(turned[:, 0:1] / full + EPSILON)
    cot = cot_ref[...].astype(FLOAT)
    normed = emb_ref[...].astype(FLOAT) * inverse
    grad = cot * own_gain(gain_ref, place_ref[0], columns)
    out_ref[:tokens, :] = (
        (grad - normed * (turned[:, 1:2] * inverse / full)) * inverse
    ).astype(HALF)
    part = total[:, 2 * tokens :] + jnp.sum(cot * normed, axis=0, keepdims=True)
    terms = cast_pieces(part) + cast_pieces(draw_ref[...])
    out_ref[tokens:, :] = stacked_lines(terms, EXTRA_ROWS, columns).astype(HALF)


def gain_kernel(replicas, *refs):
    tokens = refs[0].shape[0] - EXTRA_ROWS
    total = jnp.zeros(refs[-1].shape, FLOAT)
    for ref in refs[:-1]:
        extra = ref[tokens:, :].astype(FLOAT)
        total = total + (extra[0:1] + extra[1:2] + extra[2:3])
    refs[-1][...] = total / replicas


def quantized_sum(tiles, meta, loads, slots, replicas, total, last):
    rows = tiles.shape[0]
    columns = loads[0].shape[1]
    adds = total is not None
    chunks = 5 if last and rows % 200 == 0 else 1
    return pl.pallas_call(
        functools.partial(quantize_kernel, slots, replicas, adds, chunks),
        in_specs=[whole()] * (len(slots) + 2 + adds),
        out_specs=anywhere() if chunks > 1 else whole(),
        out_shape=jax.ShapeDtypeStruct((rows, columns), FLOAT),
        scratch_shapes=[
            pltpu.VMEM((rows, columns), FLOAT),
            pltpu.VMEM((8, columns), FLOAT),
            pltpu.VMEM((rows, 128), FLOAT),
            pltpu.VMEM((rows, 128), FLOAT),
            pltpu.VMEM((rows, 128), FLOAT),
        ]
        + (
            [pltpu.VMEM((rows, columns), FLOAT), pltpu.SemaphoreType.DMA((chunks,))]
            if chunks > 1
            else []
        ),
        compiler_params=grant(12),
        cost_estimate=pl.CostEstimate(
            flops=len(slots) * rows * columns * 1200, bytes_accessed=0, transcendentals=0
        ),
    )(tiles, meta, *loads, *([total] if adds else []))


def half_of(value, bit, taken):
    shape = value.shape
    high = shape[0] // (2 * bit)
    cut = value.reshape((high, 2, bit) + shape[1:])[:, taken]
    return cut.reshape((high * bit,) + shape[1:])


def on_device(
    tile_tokens,
    proj_weight,
    text_hidden,
    cotangent,
    norm_gain,
    placeholders,
    bucket_levels,
    row_draws,
    column_draws,
):
    seq_count = lax.axis_size("seq")
    seq_index = lax.axis_index("seq")
    replicas = lax.axis_size("dp")
    replica = lax.axis_index("dp")
    levels_of_bits = replicas.bit_length() - 1
    assert replicas == 1 << levels_of_bits
    places = placeholders[0]
    image_total = places.shape[0]
    tok_rows, model_width = text_hidden.shape[1:]
    tile_rows, vision = tile_tokens.shape[1:]
    width, columns = proj_weight.shape
    padded = -(-width // 16) * 16
    kept_labels = tuple(range(0, replicas, 2))
    order = kept_labels + tuple(exchanged_label(label, levels_of_bits) ^ 1 for label in kept_labels)
    here = replica.astype(jnp.int32).reshape(1)
    there = seq_index.astype(jnp.int32).reshape(1)

    packed = pl.pallas_call(
        pack_kernel,
        in_specs=[anywhere()] * 3,
        out_specs=whole(),
        scratch_shapes=[
            pltpu.VMEM((tile_rows, vision), HALF),
            pltpu.VMEM((1, vision), jnp.int32),
            pltpu.VMEM((1, vision), FLOAT),
            pltpu.SemaphoreType.DMA((3,)),
        ],
        out_shape=jax.ShapeDtypeStruct((replicas, tile_rows + META_ROWS, width), HALF),
        compiler_params=grant(60),
    )(tile_tokens[0], bucket_levels[0], row_draws[0])
    exchanged = lax.all_to_all(packed, "dp", 0, 0, tiled=True)
    own_tile, meta = pl.pallas_call(
        functools.partial(unpack_kernel, order),
        in_specs=[scalar(), whole()],
        out_specs=[whole(), whole()],
        out_shape=[
            jax.ShapeDtypeStruct((padded, replicas * tile_rows), HALF),
            jax.ShapeDtypeStruct((padded, lanes(2 * replicas)), FLOAT),
        ],
        scratch_shapes=[
            pltpu.VMEM((lanes(replicas * tile_rows), lanes(width)), FLOAT),
            pltpu.VMEM((lanes(2 * replicas), lanes(width)), FLOAT),
        ],
        compiler_params=grant(8),
    )(here, exchanged)
    tile_blocks = [own_tile]
    for step in range(1, seq_count):
        low = step & -step
        tile_blocks.append(swap(tile_blocks[step ^ low], low))

    text_call = pl.pallas_call(
        text_kernel,
        in_specs=[scalar()] + [whole()] * 2 + [anywhere()] * 2,
        out_specs=[whole()] * 2,
        scratch_shapes=[
            pltpu.VMEM((tok_rows, model_width), HALF),
            pltpu.VMEM((tok_rows, model_width), HALF),
            pltpu.SemaphoreType.DMA((2 * seq_count,)),
        ],
        out_shape=[
            jax.ShapeDtypeStruct((seq_count, IMG_MOST, columns), HALF),
            jax.ShapeDtypeStruct((seq_count, 1, columns), FLOAT),
        ],
        cost_estimate=pl.CostEstimate(
            flops=tok_rows * model_width * 4000, bytes_accessed=0, transcendentals=0
        ),
        compiler_params=grant(60),
    )
    outgoing, text_parts = text_call(
        there, placeholders, places.reshape(image_total, 1), text_hidden[0], cotangent[0]
    )

    weight = jnp.pad(proj_weight, ((0, padded - width), (0, 0)))
    even = (replicas // 2) * tile_rows
    split = seq_count // 2
    parts = [tile_blocks[:split]] + [[block] for block in tile_blocks[split:]]
    sizes, summands = [], []
    for part, group in enumerate(parts):

        def product(cut, kind):
            left = jnp.concatenate([block[:, cut] for block in group], axis=1)
            out = lax.dot_general(
                left, weight, (((0,), (0,)), ((), ())), preferred_element_type=FLOAT
            ).astype(kind)
            out = out.reshape(len(group), replicas // 2, tile_rows, columns)
            return jnp.transpose(out, (1, 0, 2, 3))

        sent = product(slice(even, 2 * even), HALF)
        held = product(slice(0, even), FLOAT)
        if part == 0:
            outgoing, sent = lax.optimization_barrier((outgoing, sent))
            returned = [outgoing[0]]
            for step in range(1, seq_count):
                returned.append(swap(outgoing[step], step))
        arrived = flip(sent, 0)
        held = held + arrived.astype(FLOAT)
        if levels_of_bits == 3 and part > 0:
            sums = [held[0]]
            for place in (1, 2, 3):
                sent = held[place].astype(HALF)
                sums.append(
                    flip_label(sent, place) if place < 3 else flip_far(sent)
                )
        else:
            for bit in range(1, levels_of_bits):
                sent = half_of(held, 1, 1).astype(HALF)
                held = half_of(held, 1, 0)
                arrived = flip_label(sent, bit)
                if bit < levels_of_bits - 1:
                    held = held + arrived.astype(FLOAT)
            sums = [held, arrived]
        sizes.append(len(sums))
        summands += [value.reshape(-1, columns) for value in sums]
    tokens_of = (image_total, columns)
    middle = pl.pallas_call(
        functools.partial(middle_kernel, tuple(sizes), seq_count, tok_rows),
        in_specs=[scalar()] + [whole()] * (3 + len(summands) + seq_count),
        out_specs=[whole()] * (2 + seq_count),
        out_shape=[
            jax.ShapeDtypeStruct(tokens_of, HALF),
            jax.ShapeDtypeStruct(tokens_of, HALF),
        ]
        + [jax.ShapeDtypeStruct((1, 2 * image_total + columns), FLOAT)] * seq_count,
        compiler_params=grant(16),
    )(there, placeholders, norm_gain.reshape(1, -1), text_parts, *summands, *returned)
    embedded, image_cot = middle[:2]
    stats = [middle[2]]
    for step in range(1, seq_count):
        stats.append(swap(middle[2 + step], step))
    own_load = pl.pallas_call(
        functools.partial(finish_kernel, seq_count, model_width),
        in_specs=[scalar()] + [whole()] * (4 + seq_count),
        out_specs=whole(),
        out_shape=jax.ShapeDtypeStruct((image_total + EXTRA_ROWS, columns), HALF),
        scratch_shapes=[pltpu.VMEM((128, image_total), FLOAT)],
        compiler_params=grant(12),
    )(there, norm_gain.reshape(1, -1), embedded, image_cot, column_draws, *stats)

    regroup = pl.pallas_call(
        functools.partial(regroup_kernel, order, tile_rows),
        in_specs=[whole()] * seq_count,
        out_specs=whole(),
        out_shape=jax.ShapeDtypeStruct((padded, replicas * image_total), HALF),
        cost_estimate=pl.CostEstimate(
            flops=replicas * padded * image_total * 2000, bytes_accessed=0, transcendentals=0
        ),
        compiler_params=grant(8),
    )
    tiles = regroup(*tile_blocks)

    loads = {0: own_load}
    if levels_of_bits == 3:
        loads[1] = flip(own_load, 0)
        loads[2] = flip_label(own_load, 1)
        loads[5] = flip(loads[2], 0)
        loads[4] = flip_label(own_load, 2)
        loads[3] = flip(loads[4], 0)
        loads[6] = flip_label(loads[2], 2)
        loads[7] = flip(loads[6], 0)
        batches = ((0, 1), (2,), (5,), (4,), (3,), (6,), (7,))
    else:
        for bit in range(1, levels_of_bits):
            for slot, load in list(loads.items()):
                loads[slot ^ (1 << bit)] = flip_label(load, bit)
        for slot, load in list(loads.items()):
            loads[exchanged_label(slot, levels_of_bits) ^ 1] = flip(load, 0)
        batches = tuple((slot, slot + 1) for slot in range(0, replicas, 2))
    gain_row = pl.pallas_call(
        functools.partial(gain_kernel, replicas),
        in_specs=[whole()] * replicas,
        out_specs=whole(),
        out_shape=jax.ShapeDtypeStruct((1, columns), FLOAT),
        compiler_params=grant(12),
    )(*[loads[slot] for slot in range(replicas)])
    gains = [gain_row]
    for step in range(1, seq_count):
        gains.append(swap(gain_row, step))
    total = None
    for slots in batches:
        total = quantized_sum(
            tiles, meta, [loads[slot] for slot in slots], slots, replicas, total, slots == batches[-1]
        )
    sources = jnp.arange(seq_count, dtype=jnp.int32) ^ there
    gain_total = jnp.take(jnp.concatenate(gains, axis=0), sources, axis=0)
    return total[:width], gain_total.reshape(model_width)


def solution(mesh):
    return jax.shard_map(
        on_device,
        mesh=mesh,
        in_specs=(
            P("dp", "seq", None),
            P("dp", "seq"),
            P("dp", "seq", None),
            P("dp", "seq", None),
            P(),
            P("dp", None),
            P("dp", "seq", None),
            P("dp", "seq", None),
            P("dp", "seq"),
        ),
        out_specs=(P("dp", "seq"), P()),
        check_vma=False,
    )
```
